32 devices in a mesh: grp: 2 (over y), row: 4 (over z), col: 2 (over x), slc: 2 (over core).
Axes of the slice: x: 2, y: 2, z: 4, core: 2. Of those that a mesh axis runs over, the one named last changes fastest.
Arguments:
- objects: bfloat16 [2, 2, 3072, 768], P(None, None, ('grp', 'row'), 'col'), parts along dimension 2, may hold values from -1 to 1
- probes: bfloat16 [4, 2, 256, 256], P(('grp', 'slc')), parts along dimension 0, may hold values from -3 to 3
- weights: float32 [256, 256], replicated, may hold values from 0.1 to 1
- counts: int32 [8, 2], P(('grp', 'row'), 'col'), parts along dimension 0, may hold values from 1 to 2, as said below
- offsets: int32 [8, 2, 2, 2], P(('grp', 'row'), 'col'), parts along dimension 0, may hold values from 0 to 383, as said below
- intensities: bfloat16 [8, 2, 2, 256, 256], P(('grp', 'row'), 'col'), parts along dimension 0, may hold values from 0.049804688 to 2
Outputs:
- gradient: float32 [2, 2, 3072, 768], P('slc', None, ('grp', 'row'), 'col'), parts along dimension 2
The draws below stay inside these ranges and needn't reach their ends.
There are 2 independent parts, one for each index of `grp`. The reference program is written for one: setup_inputs(seed, part) draws one part's arguments, and reference() takes and returns one part's arrays. A program takes and returns all parts, laid end to end along the dimension named above; an argument that names none is the same for every part. Nothing has to cross between parts.
Inputs may be any that keep to these rules, and one draw needn't show every extreme that they name: `counts`: some tile has exactly 2 positions. `offsets`: every window of a live position lies inside the object; entries of slots at or after a tile's count are ignored.
All inputs are finite; a program needn't handle non-finite values.
Results may differ from the reference program's by a relative error of at most 0.019.
Values may be sent and summed in bfloat16 or wider, within the bound.
No kernel may reach another device: no remote copies, remote signals or barrier semaphores. Data moves between devices by JAX's collectives and lax.ppermute only.
A program may use at most 64 MiB of HBM per device.

```python
import math
import jax
import jax.numpy as jnp
from jax import lax

WIN = 256
TILE = 384
SLOTS = 2
SLICES = 2
MODES = 2
NY = 1536
NX = 768
N_ROW = 4
N_COL = 2


def draw_counts(key, part):
    earlier_key = jax.random.fold_in(key, 11)
    another_key = jax.random.fold_in(key, 12)
    picked_key = jax.random.fold_in(key, 13)
    earlier = jax.random.randint(earlier_key, (N_ROW, N_COL), 1, SLOTS + 1)
    another = jax.random.randint(another_key, (N_ROW, N_COL), 1, SLOTS + 1)
    lowest = jnp.minimum(earlier, another)
    picked = jax.random.randint(picked_key, (), 0, N_ROW * N_COL)
    places = jnp.arange(N_ROW * N_COL, dtype=jnp.int32).reshape(N_ROW, N_COL)
    return jnp.where(places == picked, SLOTS, lowest).astype(jnp.int32)


def draw_offsets(key, part):
    tile_rows = jnp.arange(N_ROW, dtype=jnp.int32)[:, None, None, None]
    tile_cols = jnp.arange(N_COL, dtype=jnp.int32)[None, :, None, None]
    component = jnp.arange(2, dtype=jnp.int32)[None, None, None, :]
    last_row = (tile_rows == N_ROW - 1) & (component == 0)
    last_col = (tile_cols == N_COL - 1) & (component == 1)
    ceiling = jnp.where(last_row | last_col, TILE - WIN + 1, TILE)
    ceiling = jnp.broadcast_to(ceiling, (N_ROW, N_COL, SLOTS, 2))
    return jax.random.randint(jax.random.fold_in(key, 21), (N_ROW, N_COL, SLOTS, 2), 0, ceiling).astype(jnp.int32)


def steps_of(key, shape, shards, least, top_value):
    def one(position, shards_of):
        heights = jax.random.uniform(jax.random.fold_in(jax.random.fold_in(key, 6), position), (shards_of,), jnp.float32, least / len(shards), top_value / len(shards))
        return jnp.repeat(jnp.exp(heights), shape[position] // shards_of).reshape((-1,) + (1,) * (len(shape) - position - 1))

    gain = one(*shards[0])
    for cut in shards[1:]:
        gain = gain * one(*cut)
    return gain


def noise(rng, shape, deviation, most, pieces=(), held_as=jnp.bfloat16):
    loudness = steps_of(rng, shape, pieces, -0.22, 0.18) if pieces else 1.0
    entries = jax.random.normal(rng, shape, jnp.float32) * deviation * loudness
    return jnp.minimum(jnp.maximum(entries, -most), most).astype(held_as)


def setup_inputs(seed: int = 0, part: int = 0) -> dict:
    key_list = jax.random.split(jax.random.key(seed), 7)
    part_splits = jax.random.split(jax.random.fold_in(key_list[6], part), 7)
    return {
        "objects": jnp.clip(jax.random.uniform(part_splits[0], (SLICES, 2, NY, NX), jnp.float32, -1.0, 1.0) * steps_of(part_splits[0], (SLICES, 2, NY, NX), ((2, 4), (3, 2)), -0.4, 0.0), -1.0, 1.0).astype(jnp.bfloat16),
        "probes": noise(part_splits[1], (MODES, 2, WIN, WIN), 0.5, 3.0, ((0, 2),)),
        "weights": jnp.clip(jnp.exp(jax.random.uniform(key_list[2], (WIN, WIN), jnp.float32, math.log(0.1), math.log(1.0))), 0.1, 1.0),
        "counts": draw_counts(jax.random.fold_in(jax.random.fold_in(key_list[6], part), 71), part),
        "offsets": draw_offsets(jax.random.fold_in(jax.random.fold_in(key_list[6], part), 71), part),
        "intensities": jnp.clip(jnp.exp(math.log(2.0) - 3.6927934 * jax.random.uniform(part_splits[5], (N_ROW, N_COL, SLOTS, WIN, WIN), jnp.float32) ** steps_of(part_splits[5], (N_ROW, N_COL, SLOTS, WIN, WIN), ((0, 4), (1, 2)), -0.2, 0.2)), 0.049804688, 2.0).astype(jnp.bfloat16),
    }


fresnel = 0.5

def dft_tables(extent):
    counter = jnp.arange(extent, dtype=jnp.int32)
    product = counter[:, None] * counter[None, :] % extent
    angles = 2.0 * jnp.pi / extent * product.astype(jnp.float32)
    norm_scale = 1.0 / jnp.sqrt(jnp.asarray(extent, jnp.float32))
    table_re = (jnp.cos(angles) * norm_scale).astype(jnp.bfloat16)
    table_im = (-jnp.sin(angles) * norm_scale).astype(jnp.bfloat16)
    return (table_re, table_im)

def chirp_factor(extent):
    counter = jnp.arange(extent, dtype=jnp.int32)
    signed_freq = (counter + extent // 2) % extent - extent // 2
    squares = signed_freq[:, None] * signed_freq[:, None] + signed_freq[None, :] * signed_freq[None, :]
    angles = -jnp.pi * fresnel / extent * squares.astype(jnp.float32)
    return (jnp.cos(angles), jnp.sin(angles))

def transform(real, imag, table_re, table_im):
    real_half = real.astype(jnp.bfloat16)
    imag_half = imag.astype(jnp.bfloat16)
    mid_re = jnp.dot(table_re, real_half, preferred_element_type=jnp.float32) - jnp.dot(table_im, imag_half, preferred_element_type=jnp.float32)
    mid_im = jnp.dot(table_re, imag_half, preferred_element_type=jnp.float32) + jnp.dot(table_im, real_half, preferred_element_type=jnp.float32)
    mid_re = mid_re.astype(jnp.bfloat16)
    mid_im = mid_im.astype(jnp.bfloat16)
    out_re = jnp.dot(mid_re, table_re, preferred_element_type=jnp.float32) - jnp.dot(mid_im, table_im, preferred_element_type=jnp.float32)
    out_im = jnp.dot(mid_re, table_im, preferred_element_type=jnp.float32) + jnp.dot(mid_im, table_re, preferred_element_type=jnp.float32)
    return (out_re, out_im)

def complex_mul(left_re, left_im, right_re, right_im):
    return (left_re * right_re - left_im * right_im, left_re * right_im + left_im * right_re)

def conj_mul(left_re, left_im, right_re, right_im):
    return (left_re * right_re + left_im * right_im, left_re * right_im - left_im * right_re)

def forward_mode(probe_re, probe_im, window, tables, chirps):
    table_re, table_im, inverse_im = tables
    chirp_re, chirp_im = chirps
    first_re = window[0, 0].astype(jnp.float32)
    first_im = window[0, 1].astype(jnp.float32)
    second_re = window[1, 0].astype(jnp.float32)
    second_im = window[1, 1].astype(jnp.float32)
    psi_re, psi_im = complex_mul(probe_re, probe_im, first_re, first_im)
    spec_re, spec_im = transform(psi_re, psi_im, table_re, table_im)
    spec_re, spec_im = complex_mul(chirp_re, chirp_im, spec_re, spec_im)
    prop_re, prop_im = transform(spec_re, spec_im, table_re, inverse_im)
    exit_re, exit_im = complex_mul(prop_re, prop_im, second_re, second_im)
    far_re, far_im = transform(exit_re, exit_im, table_re, table_im)
    return (prop_re, prop_im, far_re, far_im)

def backward_mode(probe_re, probe_im, window, prop_re, prop_im, far_re, far_im, residual, tables, chirps):
    table_re, table_im, inverse_im = tables
    chirp_re, chirp_im = chirps
    second_re = window[1, 0].astype(jnp.float32)
    second_im = window[1, 1].astype(jnp.float32)
    back_re, back_im = transform(residual * far_re, residual * far_im, table_re, inverse_im)
    grad_two_re, grad_two_im = conj_mul(prop_re, prop_im, back_re, back_im)
    gprop_re, gprop_im = conj_mul(second_re, second_im, back_re, back_im)
    gspec_re, gspec_im = transform(gprop_re, gprop_im, table_re, table_im)
    gspec_re, gspec_im = conj_mul(chirp_re, chirp_im, gspec_re, gspec_im)
    gpsi_re, gpsi_im = transform(gspec_re, gspec_im, table_re, inverse_im)
    grad_one_re, grad_one_im = conj_mul(probe_re, probe_im, gpsi_re, gpsi_im)
    return jnp.stack([jnp.stack([grad_one_re, grad_one_im]), jnp.stack([grad_two_re, grad_two_im])])

def reference(objects, probes, weights, counts, offsets, intensities):
    slices = objects.shape[0]
    height = objects.shape[2]
    breadth = objects.shape[3]
    extent = probes.shape[2]
    tile_size = height // N_ROW
    table_re, table_im = dft_tables(extent)
    tables = (table_re, table_im, -table_im)
    chirps = chirp_factor(extent)
    padded = jnp.pad(objects, ((0, 0), (0, 0), (0, extent), (0, extent)))
    slot_total = N_ROW * N_COL * SLOTS
    serial = jnp.arange(slot_total, dtype=jnp.int32)
    tile_row = serial // (N_COL * SLOTS)
    tile_col = serial // SLOTS % N_COL
    slot_of = serial % SLOTS
    flat_offsets = offsets.reshape(slot_total, 2).astype(jnp.int32)
    top_rows = (tile_row * tile_size + flat_offsets[:, 0]).astype(jnp.int32)
    left_cols = (tile_col * tile_size + flat_offsets[:, 1]).astype(jnp.int32)
    alive_mask = slot_of < counts.reshape(-1)[serial // SLOTS]
    measured = intensities.reshape(slot_total, extent, extent)

    def slot_term(window, data_slot):
        forwards = []
        intensity = jnp.zeros((extent, extent), jnp.float32)
        for mode_id in range(probes.shape[0]):
            probe_re = probes[mode_id, 0].astype(jnp.float32)
            probe_im = probes[mode_id, 1].astype(jnp.float32)
            result = forward_mode(probe_re, probe_im, window, tables, chirps)
            forwards.append(result)
            intensity = intensity + result[2] * result[2] + result[3] * result[3]
        residual = 2.0 * weights * (intensity - data_slot.astype(jnp.float32))
        contrib = jnp.zeros((slices, 2, extent, extent), jnp.float32)
        for mode_id in range(probes.shape[0]):
            probe_re = probes[mode_id, 0].astype(jnp.float32)
            probe_im = probes[mode_id, 1].astype(jnp.float32)
            prop_re, prop_im, far_re, far_im = forwards[mode_id]
            contrib = contrib + backward_mode(probe_re, probe_im, window, prop_re, prop_im, far_re, far_im, residual, tables, chirps)
        return contrib

    def accumulate(gradient, inputs):
        top, left, alive, data_slot = inputs
        anchor = jnp.int32(0)
        window = lax.dynamic_slice(padded, (anchor, anchor, top, left), (slices, 2, extent, extent))
        contrib = lax.cond(alive, slot_term, lambda window_in, data_in: jnp.zeros((slices, 2, extent, extent), jnp.float32), window, data_slot)
        previous = lax.dynamic_slice(gradient, (anchor, anchor, top, left), (slices, 2, extent, extent))
        gradient = lax.dynamic_update_slice(gradient, previous + contrib, (anchor, anchor, top, left))
        return (gradient, None)
    initial = jnp.zeros((slices, 2, height + extent, breadth + extent), jnp.float32)
    gradient, _ = lax.scan(accumulate, initial, (top_rows, left_cols, alive_mask, measured))
    return gradient[:, :, :height, :breadth]
```

```python
import functools

import jax
import jax.numpy as jnp
import numpy as np
from jax import lax
from jax.experimental import pallas as pl
from jax.experimental.pallas import tpu as pltpu
from jax.sharding import PartitionSpec as P

fresnel = 0.5
VMEM = pl.BlockSpec(memory_space=pltpu.VMEM)
SMEM = pl.BlockSpec(memory_space=pltpu.SMEM)
PARAMS = pltpu.CompilerParams(vmem_limit_bytes=20 * 2**20)


def host_tables(extent):
    counter = np.arange(extent)
    angles = 2.0 * np.pi / extent * (counter[:, None] * counter[None, :] % extent)
    forward = (np.cos(angles) - 1j * np.sin(angles)) / np.sqrt(extent)
    signed = (counter + extent // 2) % extent - extent // 2
    chirp = np.exp(-1j * np.pi * fresnel / extent * signed * signed)
    carry = (np.conj(forward) * chirp[None, :]) @ forward
    parts = [carry.real, carry.imag, -carry.imag, forward.real, forward.imag, -forward.imag]
    return jnp.asarray(np.stack(parts).astype(np.float32)).astype(jnp.bfloat16)


def dot(left, right):
    return jnp.dot(left, right, preferred_element_type=jnp.float32)


def one_hot(shape, row_sign, offset):
    row = lax.broadcasted_iota(jnp.int32, shape, 0)
    col = lax.broadcasted_iota(jnp.int32, shape, 1)
    return jnp.where((row - col) * row_sign == offset, 1.0, 0.0).astype(jnp.bfloat16)


def cut_kernel(offs, objects, right, below, diag, keep, send):
    me = lax.axis_index("slc")
    tile = objects.shape[2]
    win = diag.shape[1]
    for out, slot in ((send, 1 - me), (keep, me)):
        top, left = offs[2 * slot], offs[2 * slot + 1]
        rows_own = one_hot((win, tile), -1, top)
        rows_far = one_hot((win, win), -1, top - tile)
        cols_own = one_hot((tile, win), 1, left)
        cols_far = one_hot((win, win), 1, left - tile)
        for part in range(2):
            upper = dot(objects[me, part], cols_own) + dot(right[part], cols_far)
            lower = dot(below[part], cols_own) + dot(diag[part], cols_far)
            window = dot(rows_own, upper.astype(jnp.bfloat16)) + dot(
                rows_far, lower.astype(jnp.bfloat16)
            )
            out[part] = window.astype(jnp.bfloat16)


def transform(real, imag, table_re, table_im, table_in):
    real = real.astype(jnp.bfloat16)
    imag = imag.astype(jnp.bfloat16)
    mid_re = (dot(table_re, real) + dot(table_in, imag)).astype(jnp.bfloat16)
    mid_im = (dot(table_re, imag) + dot(table_im, real)).astype(jnp.bfloat16)
    out_re = dot(mid_re, table_re) + dot(mid_im, table_in)
    out_im = dot(mid_re, table_im) + dot(mid_im, table_re)
    return out_re, out_im


def complex_mul(left_re, left_im, right_re, right_im):
    return (left_re * right_re - left_im * right_im, left_re * right_im + left_im * right_re)


def conj_mul(left_re, left_im, right_re, right_im):
    return (left_re * right_re + left_im * right_im, left_re * right_im - left_im * right_re)


def grad_kernel(
    counts, kept, got, probe_a, probe_b, weights, measured, tables, keep, send, prop, far
):
    me = lax.axis_index("slc")
    carry = (tables[0], tables[1], tables[2])
    carry_conj = (tables[0], tables[2], tables[1])
    fwd = (tables[3], tables[4], tables[5])
    inv = (tables[3], tables[5], tables[4])
    first_mine = me == 0

    def pick(part, flag):
        return jnp.where(flag, kept[part], got[part]).astype(jnp.float32)

    probes = (probe_a, probe_b)
    intensity = None
    for mode, probe in enumerate(probes):
        one_re, one_im = pick(0, first_mine), pick(1, first_mine)
        psi = complex_mul(
            probe[0].astype(jnp.float32), probe[1].astype(jnp.float32), one_re, one_im
        )
        prop_re, prop_im = transform(*psi, *carry)
        prop[mode, 0] = prop_re
        prop[mode, 1] = prop_im
        two_re, two_im = pick(0, ~first_mine), pick(1, ~first_mine)
        leave = complex_mul(prop_re, prop_im, two_re, two_im)
        far_re, far_im = transform(*leave, *fwd)
        far[mode, 0] = far_re
        far[mode, 1] = far_im
        square = far_re * far_re + far_im * far_im
        intensity = square if intensity is None else intensity + square
    residual = 2.0 * weights[...] * (intensity - measured[me].astype(jnp.float32))
    residual = jnp.where(me < counts[0], residual, 0.0)
    one_sum = two_sum = None
    for mode, probe in enumerate(probes):
        back_re, back_im = transform(residual * far[mode, 0], residual * far[mode, 1], *inv)
        two = conj_mul(prop[mode, 0], prop[mode, 1], back_re, back_im)
        two_re, two_im = pick(0, ~first_mine), pick(1, ~first_mine)
        inner = conj_mul(two_re, two_im, back_re, back_im)
        gpsi_re, gpsi_im = transform(*inner, *carry_conj)
        one = conj_mul(probe[0].astype(jnp.float32), probe[1].astype(jnp.float32), gpsi_re, gpsi_im)
        one_sum = one if one_sum is None else (one_sum[0] + one[0], one_sum[1] + one[1])
        two_sum = two if two_sum is None else (two_sum[0] + two[0], two_sum[1] + two[1])
    for part in range(2):
        keep[part] = jnp.where(first_mine, one_sum[part], two_sum[part]).astype(jnp.bfloat16)
        send[part] = jnp.where(first_mine, two_sum[part], one_sum[part]).astype(jnp.bfloat16)


def place_kernel(offs, kept, got, own, right, below, diag):
    me = lax.axis_index("slc")
    tile = own.shape[1]
    win = diag.shape[1]
    rows_own, rows_far, cols_own, cols_far = [], [], [], []
    for slot in (me, 1 - me):
        top, left = offs[2 * slot], offs[2 * slot + 1]
        rows_own.append(one_hot((tile, win), 1, top))
        rows_far.append(one_hot((win, win), 1, top - tile))
        cols_own.append(one_hot((win, tile), -1, left))
        cols_far.append(one_hot((win, win), -1, left - tile))
    for part in range(2):
        parts = (kept[part], got[part])
        upper = [dot(rows_own[n], parts[n]).astype(jnp.bfloat16) for n in range(2)]
        lower = [dot(rows_far[n], parts[n]).astype(jnp.bfloat16) for n in range(2)]
        diag[part] = (dot(lower[0], cols_far[0]) + dot(lower[1], cols_far[1])).astype(jnp.bfloat16)
        below[part] = (dot(lower[0], cols_own[0]) + dot(lower[1], cols_own[1])).astype(jnp.bfloat16)
        right[part] = (dot(upper[0], cols_far[0]) + dot(upper[1], cols_far[1])).astype(jnp.bfloat16)
        own[part] = dot(upper[0], cols_own[0]) + dot(upper[1], cols_own[1])


def join_kernel(own, left, above, diag, out):
    tile = own.shape[1]
    win = diag.shape[1]
    for part in range(2):
        out[0, part, win:, win:] = own[part, win:, win:]
        out[0, part, win:, :win] = own[part, win:, :win] + left[part, win:, :].astype(jnp.float32)
        out[0, part, :win, win:] = own[part, :win, win:] + above[part, :, win:].astype(jnp.float32)
        out[0, part, :win, :win] = (
            own[part, :win, :win]
            + left[part, :win, :].astype(jnp.float32)
            + above[part, :, :win].astype(jnp.float32)
            + diag[part].astype(jnp.float32)
        )


def body(rows, cols, objects, probes, weights, counts, offsets, intensities):
    tile = objects.shape[2]
    win = probes.shape[2]
    half = jnp.bfloat16
    me = lax.axis_index("slc")

    def shift(x, down, across):
        pairs = []
        for r in range(rows):
            for c in range(cols):
                if 0 <= r + down < rows and 0 <= c + across < cols:
                    pairs.append((r * cols + c, (r + down) * cols + c + across))
        return lax.ppermute(x, ("row", "col"), pairs)

    def swap(x):
        return lax.ppermute(x, "slc", [(0, 1), (1, 0)])

    def strip(height, width):
        zero = jnp.int32(0)
        return lax.dynamic_slice(objects, (me, zero, zero, zero), (1, 2, height, width))[0]

    right = shift(strip(tile, win), 0, -1)
    below = shift(strip(win, tile), -1, 0)
    diag = shift(strip(win, win), -1, -1)
    probe = probes[0]
    probe_other = swap(probe)
    offs = offsets.reshape(-1)
    window = jax.ShapeDtypeStruct((2, win, win), half)
    keep, send = pl.pallas_call(
        cut_kernel,
        out_shape=(window, window),
        in_specs=[SMEM] + [VMEM] * 4,
        out_specs=(VMEM, VMEM),
        compiler_params=PARAMS,
        name="cut",
    )(offs, objects, right, below, diag)
    got = swap(send)
    keep, send = pl.pallas_call(
        grad_kernel,
        out_shape=(window, window),
        in_specs=[SMEM] + [VMEM] * 7,
        out_specs=(VMEM, VMEM),
        scratch_shapes=[pltpu.VMEM((2, 2, win, win), jnp.float32)] * 2,
        compiler_params=PARAMS,
        name="grad",
    )(
        counts.reshape(-1),
        keep,
        got,
        probe,
        probe_other,
        weights,
        intensities[0, 0],
        host_tables(win),
    )
    got = swap(send)
    own, right, below, diag = pl.pallas_call(
        place_kernel,
        out_shape=(
            jax.ShapeDtypeStruct((2, tile, tile), jnp.float32),
            jax.ShapeDtypeStruct((2, tile, win), half),
            jax.ShapeDtypeStruct((2, win, tile), half),
            window,
        ),
        in_specs=[SMEM] + [VMEM] * 2,
        out_specs=(VMEM,) * 4,
        compiler_params=PARAMS,
        name="place",
    )(offs, keep, got)
    from_left = shift(right, 0, 1)
    from_above = shift(below, 1, 0)
    from_diag = shift(diag, 1, 1)
    return pl.pallas_call(
        join_kernel,
        out_shape=jax.ShapeDtypeStruct((1, 2, tile, tile), jnp.float32),
        in_specs=[VMEM] * 4,
        out_specs=VMEM,
        compiler_params=PARAMS,
        name="join",
    )(own, from_left, from_above, from_diag)


def solution(mesh):
    in_specs = (
        P(None, None, ("grp", "row"), "col"),
        P(("grp", "slc"), None, None, None),
        P(),
        P(("grp", "row"), "col"),
        P(("grp", "row"), "col", None, None),
        P(("grp", "row"), "col", None, None, None),
    )
    out_specs = P("slc", None, ("grp", "row"), "col")
    run = functools.partial(body, mesh.shape["row"], mesh.shape["col"])
    return jax.shard_map(run, mesh=mesh, in_specs=in_specs, out_specs=out_specs, check_vma=False)
```

```python
import functools

import jax
import jax.numpy as jnp
import numpy as np
from jax import lax
from jax.experimental import pallas as pl
from jax.experimental.pallas import tpu as pltpu
from jax.sharding import PartitionSpec as P


fresnel = 0.5
VMEM = pl.BlockSpec(memory_space=pltpu.VMEM)
HBM = pl.BlockSpec(memory_space=pltpu.HBM)
SMEM = pl.BlockSpec(memory_space=pltpu.SMEM)
PARAMS = pltpu.CompilerParams(vmem_limit_bytes=20 * 2**20)


def host_tables(extent):
    counter = np.arange(extent)
    angles = 2.0 * np.pi / extent * (counter[:, None] * counter[None, :] % extent)
    forward = (np.cos(angles) - 1j * np.sin(angles)) / np.sqrt(extent)
    signed = (counter + extent // 2) % extent - extent // 2
    chirp = np.exp(-1j * np.pi * fresnel / extent * signed * signed)
    carry = (np.conj(forward) * chirp[None, :]) @ forward
    parts = [carry.real, carry.imag, -carry.imag, forward.real, forward.imag, -forward.imag]
    return jnp.asarray(np.stack(parts).astype(np.float32)).astype(jnp.bfloat16)


def dot(left, right):
    return jnp.dot(left, right, preferred_element_type=jnp.float32)


def one_hot(shape, row_sign, offset):
    row = lax.broadcasted_iota(jnp.int32, shape, 0)
    col = lax.broadcasted_iota(jnp.int32, shape, 1)
    return jnp.where((row - col) * row_sign == offset, 1.0, 0.0).astype(jnp.bfloat16)


def strip_moves(tile, win):
    half, rest = win // 2, tile - win
    right = (
        (0, 0, 0, half, win, half, 0),
        (1, 0, 0, half, win, 0, 0),
        (1, half, 0, rest, win, win, 0),
    )
    below = (
        (0, 0, 0, half, win, 0, 0),
        (1, 0, 0, half, win, half, 0),
        (1, half, 0, half, rest, 0, win),
        (1, half, rest, half, rest, half, win),
    )
    return right, below


def by_core(me, run):
    for core in range(2):

        @pl.when(me == core)
        def _(core=core):
            run(core)


def strips_kernel(objects, one, two, sems):
    me = lax.axis_index("slc")
    tile = objects.shape[2]
    win = two.shape[2]

    def run(core):
        copies = []
        for move in strip_moves(tile, win)[core]:
            out, row, col, height, width, from_row, from_col = move
            copies.append(
                pltpu.make_async_copy(
                    objects.at[:, :, pl.ds(from_row, height), pl.ds(from_col, width)],
                    (one, two)[out].at[:, :, pl.ds(row, height), pl.ds(col, width)],
                    sems.at[len(copies)],
                )
            )
        for copy in copies:
            copy.start()
        for copy in copies:
            copy.wait()

    by_core(me, run)


def half_of(value):
    return value.astype(jnp.bfloat16)


def prepare_kernel(offs, objects, tall, wide, held):
    me = lax.axis_index("slc")
    tile = objects.shape[2]
    ext, win = tall.shape[2:]
    for n, slot in enumerate((me, 1 - me)):
        for dim in range(2):
            offset = offs[2 * slot + dim]
            tall[n, dim] = one_hot((ext, win), 1, offset)
            wide[n, dim] = one_hot((win, ext), -1, offset)
    for k in range(2):
        for part in range(2):
            upper = half_of(dot(objects[k, part], tall[0, 1, :tile]))
            held[k, part] = half_of(dot(wide[0, 0, :, :tile], upper))


def reach_kernel(tall, wide, held, one, two, out):
    me = lax.axis_index("slc")
    half, win = one.shape[2:]
    tile = tall.shape[2] - win
    rest = tile - win

    def run(core):
        for k in range(2):
            for part in range(2):
                first = one[k, part]
                second = two.at[k, part]
                if core == 0:
                    got = jnp.concatenate([second[:half], first, second[half:]], axis=0)
                else:
                    near = jnp.concatenate([first, second[:half]], axis=0)
                    side = jnp.concatenate([second[half:, :rest], second[half:, rest:]], axis=0)
                    got = jnp.concatenate([near, side], axis=1)
                for n in range(2):
                    if core == 0:
                        window = dot(wide[n, 0, :, :tile], half_of(dot(got, tall[n, 1, tile:])))
                    else:
                        window = dot(wide[n, 0, :, tile:], half_of(dot(got, tall[n, 1, :tile])))
                    if n == 0:
                        window = held[k, part].astype(jnp.float32) + window
                    out[n, k, part] = half_of(window)

    by_core(me, run)


def corner_kernel(tall, wide, held, three, keep, send):
    me = lax.axis_index("slc")
    half, win = three.shape[2:]
    tile = tall.shape[2] - win

    def run(core):
        start = tile + half * (1 - core)
        for n, out in ((1, send), (0, keep)):
            for k in range(2):
                for part in range(2):
                    lower = half_of(dot(three[k, part], tall[n, 1, tile:]))
                    window = dot(wide[n, 0, :, start : start + half], lower)
                    out[k, part] = half_of(held[n, k, part].astype(jnp.float32) + window)

    by_core(me, run)


def transform(real, imag, table_re, table_im, table_in):
    real = real.astype(jnp.bfloat16)
    imag = imag.astype(jnp.bfloat16)
    mid_re = (dot(table_re, real) + dot(table_in, imag)).astype(jnp.bfloat16)
    mid_im = (dot(table_re, imag) + dot(table_im, real)).astype(jnp.bfloat16)
    out_re = dot(mid_re, table_re) + dot(mid_im, table_in)
    out_im = dot(mid_re, table_im) + dot(mid_im, table_re)
    return out_re, out_im


def complex_mul(left_re, left_im, right_re, right_im):
    return (left_re * right_re - left_im * right_im, left_re * right_im + left_im * right_re)


def conj_mul(left_re, left_im, right_re, right_im):
    return (left_re * right_re + left_im * right_im, left_re * right_im - left_im * right_re)


def grad_kernel(
    counts, kept, got, probe_a, probe_b, weights, measured, tables, out, objs, prop, far
):
    me = lax.axis_index("slc")
    carry = (tables[0], tables[1], tables[2])
    carry_conj = (tables[0], tables[2], tables[1])
    fwd = (tables[3], tables[4], tables[5])
    inv = (tables[3], tables[5], tables[4])
    full = jnp.float32
    for k in range(2):
        for part in range(2):
            objs[k, part] = kept[k, part].astype(full) + got[k, part].astype(full)
    probes = (probe_a, probe_b)
    intensity = None
    for mode, probe in enumerate(probes):
        psi = complex_mul(probe[0].astype(full), probe[1].astype(full), objs[0, 0], objs[0, 1])
        prop_re, prop_im = transform(*psi, *carry)
        prop[mode, 0] = prop_re
        prop[mode, 1] = prop_im
        leave = complex_mul(prop_re, prop_im, objs[1, 0], objs[1, 1])
        far_re, far_im = transform(*leave, *fwd)
        far[mode, 0] = far_re
        far[mode, 1] = far_im
        square = far_re * far_re + far_im * far_im
        intensity = square if intensity is None else intensity + square
    residual = 2.0 * weights[...] * (intensity - measured[me].astype(full))
    residual = jnp.where(me < counts[0], residual, 0.0)
    one_sum = two_sum = None
    for mode, probe in enumerate(probes):
        back_re, back_im = transform(residual * far[mode, 0], residual * far[mode, 1], *inv)
        two = conj_mul(prop[mode, 0], prop[mode, 1], back_re, back_im)
        inner = conj_mul(objs[1, 0], objs[1, 1], back_re, back_im)
        gpsi_re, gpsi_im = transform(*inner, *carry_conj)
        one = conj_mul(probe[0].astype(full), probe[1].astype(full), gpsi_re, gpsi_im)
        one_sum = one if one_sum is None else (one_sum[0] + one[0], one_sum[1] + one[1])
        two_sum = two if two_sum is None else (two_sum[0] + two[0], two_sum[1] + two[1])
    for part in range(2):
        out[0, part] = half_of(one_sum[part])
        out[1, part] = half_of(two_sum[part])


def placed(tall, wide, grads, k, part, rows, cols):
    total = None
    for n, grad in enumerate(grads):
        left = half_of(dot(tall[n, 0, rows[0] : rows[0] + rows[1]], grad[k, part]))
        term = dot(left, wide[n, 1, :, cols[0] : cols[0] + cols[1]])
        total = term if total is None else total + term
    return total


def tip_kernel(tall, wide, kept, got, one):
    me = lax.axis_index("slc")
    half, win = one.shape[2:]
    tile = tall.shape[2] - win

    def run(core):
        for k in range(2):
            for part in range(2):
                one[k, part] = half_of(
                    placed(
                        tall,
                        wide,
                        (kept, got),
                        k,
                        part,
                        (tile + half * core, half),
                        (tile, win),
                    )
                )

    by_core(me, run)


def side_kernel(tall, wide, kept, got, two, add):
    me = lax.axis_index("slc")
    half, win = add.shape[2:]
    tile = tall.shape[2] - win
    rest = tile - win

    def run(core):
        for k in range(2):
            for part in range(2):
                put = functools.partial(placed, tall, wide, (kept, got), k, part)
                out = two.at[k, part]
                if core == 0:
                    out[:half] = half_of(put((0, half), (tile, win)))
                    out[half:] = half_of(put((win, rest), (tile, win)))
                    add[k, part] = put((tile, half), (0, win))
                else:
                    out[:half] = half_of(put((tile + half, half), (0, win)))
                    side = half_of(put((tile, win), (win, rest)))
                    out[half:, :rest] = side[:half]
                    out[half:, rest:] = side[half:]
                    add[k, part] = put((half, half), (tile, win))

    by_core(me, run)


def add_kernel(mine, got, out):
    out[...] = half_of(mine[...] + got[...].astype(jnp.float32))


def own_kernel(tall, wide, kept, got, own):
    me = lax.axis_index("slc")
    tile = own.shape[1]
    for part in range(2):
        own[part] = placed(tall, wide, (kept, got), me, part, (0, tile), (0, tile))


def join_kernel(own, two_mine, two_other, three_mine, three_other, out):
    me = lax.axis_index("slc")
    half, win = three_mine.shape[2:]
    tile = own.shape[1]
    rest = tile - win
    full = jnp.float32

    def run(core):
        x_two, z_two = (two_mine, two_other) if core == 0 else (two_other, two_mine)
        z_three, x_three = (three_mine, three_other) if core == 0 else (three_other, three_mine)
        for part in range(2):
            out[0, part, win:, win:] = own[part, win:, win:]
            out[0, part, win:, :win] = own[part, win:, :win] + x_two[core, part, half:].astype(full)
            out[0, part, :half, win:] = own[part, :half, win:] + z_two[
                core, part, half:, :rest
            ].astype(full)
            out[0, part, half:win, win:] = own[part, half:win, win:] + z_two[
                core, part, half:, rest:
            ].astype(full)
            out[0, part, :half, :win] = (
                own[part, :half, :win]
                + x_two[core, part, :half].astype(full)
                + z_three[core, part].astype(full)
            )
            out[0, part, half:win, :win] = (
                own[part, half:win, :win]
                + x_three[core, part].astype(full)
                + z_two[core, part, :half].astype(full)
            )

    by_core(me, run)


def call(kernel, out_shape, *args, specs=None, scratch=()):
    return pl.pallas_call(
        kernel,
        out_shape=out_shape,
        in_specs=specs or [VMEM] * len(args),
        out_specs=jax.tree.map(lambda _: VMEM, out_shape),
        scratch_shapes=scratch,
        compiler_params=PARAMS,
    )(*args)


def body(rows, cols, objects, probes, weights, counts, offsets, intensities):
    tile = objects.shape[2]
    win = probes.shape[2]
    half, ext = win // 2, tile + win
    low = jnp.bfloat16

    def shift(x, step, across):
        pairs = []
        for r in range(rows):
            for c in range(cols):
                for core in range(2):
                    down, over = (0, step) if core == across else (step, 0)
                    if 0 <= r + down < rows and 0 <= c + over < cols:
                        target = (r + down) * cols + c + over
                        pairs.append(((r * cols + c) * 2 + core, target * 2 + core))
        return lax.ppermute(x, ("row", "col", "slc"), pairs)

    def swap(x):
        return lax.ppermute(x, "slc", [(0, 1), (1, 0)])

    def shape(*dims, dtype=low):
        return jax.ShapeDtypeStruct(dims, dtype)

    offs = offsets.reshape(-1)
    quad = shape(2, 2, win, win)
    piece = shape(2, 2, half, win)
    moves = max(len(moves) for moves in strip_moves(tile, win))
    one, two = call(
        strips_kernel,
        (piece, quad),
        objects,
        specs=[HBM],
        scratch=[pltpu.SemaphoreType.DMA((moves,))],
    )
    one = shift(one, -1, 0)
    two = shift(two, -1, 0)
    probe = probes[0]
    probe_other = swap(probe)
    tall, wide, held = call(
        prepare_kernel,
        (shape(2, 2, ext, win), shape(2, 2, win, ext), quad),
        offs,
        objects,
        specs=[SMEM, VMEM],
    )
    three = shift(one, -1, 1)
    held = call(reach_kernel, shape(2, 2, 2, win, win), tall, wide, held, one, two)
    keep, send = call(corner_kernel, (quad, quad), tall, wide, held, three)
    got = swap(send)
    grads = call(
        grad_kernel,
        quad,
        counts.reshape(-1),
        keep,
        got,
        probe,
        probe_other,
        weights,
        intensities[0, 0],
        host_tables(win),
        specs=[SMEM] + [VMEM] * 7,
        scratch=[pltpu.VMEM((2, 2, win, win), jnp.float32)] * 3,
    )
    got = swap(grads)
    one = shift(call(tip_kernel, piece, tall, wide, grads, got), 1, 0)
    addend = shape(2, 2, half, win, dtype=jnp.float32)
    two, add = call(side_kernel, (quad, addend), tall, wide, grads, got)
    two = shift(two, 1, 0)
    three = shift(call(add_kernel, piece, add, one), 1, 1)
    own = call(own_kernel, shape(2, tile, tile, dtype=jnp.float32), tall, wide, grads, got)
    return call(
        join_kernel,
        shape(1, 2, tile, tile, dtype=jnp.float32),
        own,
        two,
        swap(two),
        three,
        swap(three),
    )


def staged(rows, cols, *args):
    return body(rows, cols, *args)


def solution(mesh):
    in_specs = (
        P(None, None, ("grp", "row"), "col"),
        P(("grp", "slc"), None, None, None),
        P(),
        P(("grp", "row"), "col"),
        P(("grp", "row"), "col", None, None),
        P(("grp", "row"), "col", None, None, None),
    )
    out_specs = P("slc", None, ("grp", "row"), "col")
    run = functools.partial(staged, mesh.shape["row"], mesh.shape["col"])
    return jax.shard_map(run, mesh=mesh, in_specs=in_specs, out_specs=out_specs, check_vma=False)
```

```python
import functools

import jax
import jax.numpy as jnp
import numpy as np
from jax import lax
from jax.experimental import pallas as pl
from jax.experimental.pallas import tpu as pltpu
from jax.sharding import PartitionSpec as P


fresnel = 0.5
VMEM = pl.BlockSpec(memory_space=pltpu.VMEM)
HBM = pl.BlockSpec(memory_space=pltpu.HBM)
SMEM = pl.BlockSpec(memory_space=pltpu.SMEM)
PARAMS = pltpu.CompilerParams(vmem_limit_bytes=20 * 2**20)


def host_tables(extent):
    counter = np.arange(extent)
    angles = 2.0 * np.pi / extent * (counter[:, None] * counter[None, :] % extent)
    forward = (np.cos(angles) - 1j * np.sin(angles)) / np.sqrt(extent)
    signed = (counter + extent // 2) % extent - extent // 2
    chirp = np.exp(-1j * np.pi * fresnel / extent * signed * signed)
    carry = (np.conj(forward) * chirp[None, :]) @ forward
    parts = [carry.real, carry.imag, -carry.imag, forward.real, forward.imag, -forward.imag]
    return jnp.asarray(np.stack(parts).astype(np.float32)).astype(jnp.bfloat16)


def dot(left, right):
    return jnp.dot(left, right, preferred_element_type=jnp.float32)


def one_hot(shape, row_sign, offset):
    row = lax.broadcasted_iota(jnp.int32, shape, 0)
    col = lax.broadcasted_iota(jnp.int32, shape, 1)
    return jnp.where((row - col) * row_sign == offset, 1.0, 0.0).astype(jnp.bfloat16)


def strip_moves(tile, win):
    half, rest = win // 2, tile - win
    return (
        ((half, win), ((0, 0, half, win, 0, 0),)),
        ((half, win), ((0, 0, half, win, half, 0),)),
        (
            (win, win),
            (
                (0, 0, half, win, half, 0),
                (half, 0, half, rest, 0, win),
                (half, rest, half, rest, half, win),
            ),
        ),
        ((win, win), ((0, 0, half, win, 0, 0), (half, 0, rest, win, win, 0))),
    )


def strips_kernel(strips, objects, *refs):
    me = lax.axis_index("slc")
    sems = refs[-1]
    copies = []
    for (_, moves), out in zip(strips, refs):
        for row, col, height, width, from_row, from_col in moves:
            copies.append(
                pltpu.make_async_copy(
                    objects.at[me, :, pl.ds(from_row, height), pl.ds(from_col, width)],
                    out.at[:, pl.ds(row, height), pl.ds(col, width)],
                    sems.at[len(copies)],
                )
            )
    for copy in copies:
        copy.start()
    for copy in copies:
        copy.wait()


def half_of(value):
    return value.astype(jnp.bfloat16)


def prepare_kernel(offs, objects, tall, wide, held):
    me = lax.axis_index("slc")
    tile = objects.shape[2]
    ext, win = tall.shape[2:]
    for n, slot in enumerate((me, 1 - me)):
        for dim in range(2):
            offset = offs[2 * slot + dim]
            tall[n, dim] = one_hot((ext, win), 1, offset)
            wide[n, dim] = one_hot((win, ext), -1, offset)
        for part in range(2):
            upper = half_of(dot(objects[me, part], tall[n, 1, :tile]))
            held[n, part] = half_of(dot(wide[n, 0, :, :tile], upper))


def reach_kernel(tall, wide, held, x_one, x_two, z_one, z_two, out):
    half, win = x_one.shape[1:]
    tile = tall.shape[2] - win
    rest = tile - win
    for part in range(2):
        right = jnp.concatenate([x_two[part, :half], x_one[part], x_two[part, half:]], axis=0)
        near = jnp.concatenate([z_one[part], z_two[part, :half]], axis=0)
        side = jnp.concatenate([z_two[part, half:, :rest], z_two[part, half:, rest:]], axis=0)
        below = jnp.concatenate([near, side], axis=1)
        for n in range(2):
            upper = half_of(dot(right, tall[n, 1, tile:]))
            lower = half_of(dot(below, tall[n, 1, :tile]))
            window = dot(wide[n, 0, :, :tile], upper) + dot(wide[n, 0, :, tile:], lower)
            out[n, part] = half_of(held[n, part].astype(jnp.float32) + window)


def corner_kernel(tall, wide, held, x_three, z_three, keep, send):
    win = keep.shape[1]
    tile = tall.shape[2] - win
    for n, out in ((1, send), (0, keep)):
        for part in range(2):
            corner = jnp.concatenate([x_three[part], z_three[part]], axis=0)
            lower = half_of(dot(corner, tall[n, 1, tile:]))
            window = dot(wide[n, 0, :, tile:], lower)
            out[part] = half_of(held[n, part].astype(jnp.float32) + window)


def transform(real, imag, table_re, table_im, table_in):
    real = real.astype(jnp.bfloat16)
    imag = imag.astype(jnp.bfloat16)
    mid_re = (dot(table_re, real) + dot(table_in, imag)).astype(jnp.bfloat16)
    mid_im = (dot(table_re, imag) + dot(table_im, real)).astype(jnp.bfloat16)
    out_re = dot(mid_re, table_re) + dot(mid_im, table_in)
    out_im = dot(mid_re, table_im) + dot(mid_im, table_re)
    return out_re, out_im


def complex_mul(left_re, left_im, right_re, right_im):
    return (left_re * right_re - left_im * right_im, left_re * right_im + left_im * right_re)


def conj_mul(left_re, left_im, right_re, right_im):
    return (left_re * right_re + left_im * right_im, left_re * right_im - left_im * right_re)


def grad_kernel(
    counts, kept, got, probe_a, probe_b, weights, measured, tables, keep, send, prop, far
):
    me = lax.axis_index("slc")
    carry = (tables[0], tables[1], tables[2])
    carry_conj = (tables[0], tables[2], tables[1])
    fwd = (tables[3], tables[4], tables[5])
    inv = (tables[3], tables[5], tables[4])
    first_mine = me == 0

    def pick(part, flag):
        return jnp.where(flag, kept[part], got[part]).astype(jnp.float32)

    probes = (probe_a, probe_b)
    intensity = None
    for mode, probe in enumerate(probes):
        one_re, one_im = pick(0, first_mine), pick(1, first_mine)
        psi = complex_mul(
            probe[0].astype(jnp.float32), probe[1].astype(jnp.float32), one_re, one_im
        )
        prop_re, prop_im = transform(*psi, *carry)
        prop[mode, 0] = prop_re
        prop[mode, 1] = prop_im
        two_re, two_im = pick(0, ~first_mine), pick(1, ~first_mine)
        leave = complex_mul(prop_re, prop_im, two_re, two_im)
        far_re, far_im = transform(*leave, *fwd)
        far[mode, 0] = far_re
        far[mode, 1] = far_im
        square = far_re * far_re + far_im * far_im
        intensity = square if intensity is None else intensity + square
    residual = 2.0 * weights[...] * (intensity - measured[me].astype(jnp.float32))
    residual = jnp.where(me < counts[0], residual, 0.0)
    one_sum = two_sum = None
    for mode, probe in enumerate(probes):
        back_re, back_im = transform(residual * far[mode, 0], residual * far[mode, 1], *inv)
        two = conj_mul(prop[mode, 0], prop[mode, 1], back_re, back_im)
        two_re, two_im = pick(0, ~first_mine), pick(1, ~first_mine)
        inner = conj_mul(two_re, two_im, back_re, back_im)
        gpsi_re, gpsi_im = transform(*inner, *carry_conj)
        one = conj_mul(probe[0].astype(jnp.float32), probe[1].astype(jnp.float32), gpsi_re, gpsi_im)
        one_sum = one if one_sum is None else (one_sum[0] + one[0], one_sum[1] + one[1])
        two_sum = two if two_sum is None else (two_sum[0] + two[0], two_sum[1] + two[1])
    for part in range(2):
        keep[part] = jnp.where(first_mine, one_sum[part], two_sum[part]).astype(jnp.bfloat16)
        send[part] = jnp.where(first_mine, two_sum[part], one_sum[part]).astype(jnp.bfloat16)


def tip_kernel(tall, wide, kept, got, low, x_one, z_one):
    half, win = x_one.shape[1:]
    tile = tall.shape[2] - win
    for part in range(2):
        corner = None
        for n, grad in enumerate((kept, got)):
            lower = half_of(dot(tall[n, 0, tile:], grad[part]))
            low[n, part] = lower
            term = dot(lower, wide[n, 1, :, tile:])
            corner = term if corner is None else corner + term
        x_one[part] = half_of(corner[:half])
        z_one[part] = half_of(corner[half:])


def side_kernel(tall, wide, kept, got, low, up, x_add, z_add, x_two, z_two):
    half, win = x_add.shape[1:]
    tile = tall.shape[2] - win
    rest = tile - win
    for part in range(2):
        right = below = None
        for n, grad in enumerate((kept, got)):
            upper = half_of(dot(tall[n, 0, :tile], grad[part]))
            up[n, part] = upper
            far = dot(upper, wide[n, 1, :, tile:])
            near = dot(low[n, part], wide[n, 1, :, :tile])
            right = far if right is None else right + far
            below = near if below is None else below + near
        x_two[part, :half] = half_of(right[:half])
        x_two[part, half:] = half_of(right[win:])
        x_add[part] = right[half:win]
        z_add[part] = below[:half, :win]
        z_two[part, :half] = half_of(below[half:, :win])
        z_two[part, half:, :rest] = half_of(below[:half, win:])
        z_two[part, half:, rest:] = half_of(below[half:, win:])


def add_kernel(mine, got, out):
    out[...] = half_of(mine[...] + got[...].astype(jnp.float32))


def own_kernel(wide, up, own):
    tile = own.shape[1]
    for part in range(2):
        own[part] = dot(up[0, part], wide[0, 1, :, :tile]) + dot(up[1, part], wide[1, 1, :, :tile])


def join_kernel(own, x_two, x_three, z_two, z_three, out):
    half, win = x_three.shape[1:]
    rest = own.shape[1] - win
    full = jnp.float32
    for part in range(2):
        out[0, part, win:, win:] = own[part, win:, win:]
        out[0, part, win:, :win] = own[part, win:, :win] + x_two[part, half:].astype(full)
        out[0, part, :half, win:] = own[part, :half, win:] + z_two[part, half:, :rest].astype(full)
        out[0, part, half:win, win:] = own[part, half:win, win:] + z_two[
            part, half:, rest:
        ].astype(full)
        out[0, part, :half, :win] = (
            own[part, :half, :win] + x_two[part, :half].astype(full) + z_three[part].astype(full)
        )
        out[0, part, half:win, :win] = (
            own[part, half:win, :win] + x_three[part].astype(full) + z_two[part, :half].astype(full)
        )


def call(kernel, out_shape, *args, specs=None, scratch=()):
    return pl.pallas_call(
        kernel,
        out_shape=out_shape,
        in_specs=specs or [VMEM] * len(args),
        out_specs=jax.tree.map(lambda _: VMEM, out_shape),
        scratch_shapes=scratch,
        compiler_params=PARAMS,
    )(*args)


def body(rows, cols, objects, probes, weights, counts, offsets, intensities):
    tile = objects.shape[2]
    win = probes.shape[2]
    half, ext = win // 2, tile + win
    low = jnp.bfloat16

    def shift(x, down, across):
        pairs = []
        for r in range(rows):
            for c in range(cols):
                pairs.append((r * cols + c, (r + down) % rows * cols + (c + across) % cols))
        return lax.ppermute(x, ("row", "col"), pairs)

    def swap(x):
        return lax.ppermute(x, "slc", [(0, 1), (1, 0)])

    def shape(*dims, dtype=low):
        return jax.ShapeDtypeStruct(dims, dtype)

    offs = offsets.reshape(-1)
    window = shape(2, win, win)
    strips = strip_moves(tile, win)
    z_one, x_one, z_two, x_two = call(
        functools.partial(strips_kernel, strips),
        tuple(shape(2, *dims) for dims, _ in strips),
        objects,
        specs=[HBM],
        scratch=[pltpu.SemaphoreType.DMA((sum(len(moves) for _, moves in strips),))],
    )
    z_one = shift(z_one, -1, 0)
    x_one = shift(x_one, 0, -1)
    z_two = shift(z_two, -1, 0)
    x_two = shift(x_two, 0, -1)
    probe = probes[0]
    probe_other = swap(probe)
    tall, wide, held = call(
        prepare_kernel,
        (shape(2, 2, ext, win), shape(2, 2, win, ext), shape(2, 2, win, win)),
        offs,
        objects,
        specs=[SMEM, VMEM],
    )
    x_three = shift(z_one, 0, -1)
    z_three = shift(x_one, -1, 0)
    held = call(reach_kernel, shape(2, 2, win, win), tall, wide, held, x_one, x_two, z_one, z_two)
    keep, send = call(corner_kernel, (window, window), tall, wide, held, x_three, z_three)
    got = swap(send)
    keep, send = call(
        grad_kernel,
        (window, window),
        counts.reshape(-1),
        keep,
        got,
        probe,
        probe_other,
        weights,
        intensities[0, 0],
        host_tables(win),
        specs=[SMEM] + [VMEM] * 7,
        scratch=[pltpu.VMEM((2, 2, win, win), jnp.float32)] * 2,
    )
    got = swap(send)
    piece = shape(2, half, win)
    lower, x_one, z_one = call(
        tip_kernel, (shape(2, 2, win, win), piece, piece), tall, wide, keep, got
    )
    x_one = shift(x_one, 0, 1)
    z_one = shift(z_one, 1, 0)
    addend = shape(2, half, win, dtype=jnp.float32)
    upper, x_add, z_add, x_two, z_two = call(
        side_kernel,
        (shape(2, 2, tile, win), addend, addend, window, window),
        tall,
        wide,
        keep,
        got,
        lower,
    )
    x_two = shift(x_two, 0, 1)
    z_two = shift(z_two, 1, 0)
    z_three = shift(call(add_kernel, piece, z_add, x_one), 1, 0)
    x_three = shift(call(add_kernel, piece, x_add, z_one), 0, 1)
    own = call(own_kernel, shape(2, tile, tile, dtype=jnp.float32), wide, upper)
    return call(
        join_kernel, shape(1, 2, tile, tile, dtype=jnp.float32), own, x_two, x_three, z_two, z_three
    )


def staged(rows, cols, *args):
    return body(rows, cols, *args)


def solution(mesh):
    in_specs = (
        P(None, None, ("grp", "row"), "col"),
        P(("grp", "slc"), None, None, None),
        P(),
        P(("grp", "row"), "col"),
        P(("grp", "row"), "col", None, None),
        P(("grp", "row"), "col", None, None, None),
    )
    out_specs = P("slc", None, ("grp", "row"), "col")
    run = functools.partial(staged, mesh.shape["row"], mesh.shape["col"])
    return jax.shard_map(run, mesh=mesh, in_specs=in_specs, out_specs=out_specs, check_vma=False)
```
